256 devices in a mesh: grp: 2 (over z), trn: 64 (over y, x), tst: 2 (over core).
Axes of the slice: x: 8, y: 8, z: 2, core: 2. Of those that a mesh axis runs over, the one named last changes fastest.
The devices are a block of a 8x8x16 slice.
Arguments:
- test_points: bfloat16 [64, 8192], P(None, ('grp', 'tst')), parts along dimension 1, may hold values from -9 to 9
- train_points: bfloat16 [64, 524288], P(None, ('grp', 'trn')), parts along dimension 1, may hold values from -6 to 6
- weights: bfloat16 [524288], P(('grp', 'trn')), parts along dimension 0, may hold values from -6 to 6
- factor: bfloat16 [524288, 512], P(('grp', 'trn')), parts along dimension 0, may hold values from -1.14904852 to 1.14904852
Outputs:
- mean: float32 [8192], P(('grp', 'tst')), parts along dimension 0
- variance: float32 [8192], P(('grp', 'tst')), parts along dimension 0
The draws below stay inside these ranges and needn't reach their ends.
There are 2 independent parts, one for each index of `grp`. The reference program is written for one: setup_inputs(seed, part) draws one part's arguments, and reference() takes and returns one part's arrays. A program takes and returns all parts, laid end to end along the dimension named above; each array names one. Nothing has to cross between parts.
All inputs are finite; a program needn't handle non-finite values.
Results may differ from the reference program's by a relative error of at most 0.0033.
Values sent between devices are 32-bit elements; how exact they have to be, the bound alone decides.
A program may use at most 64 MiB of HBM per device.

```python
import math
import jax
import jax.numpy as jnp
from jax import lax

DIM = 64
RANK = 512
TEST = 4096
TRAIN = 262144


def points_of(key):
    base_key = jax.random.fold_in(key, 11)
    train = jnp.clip(jax.random.normal(base_key, (DIM, TRAIN), jnp.float32), -6.0, 6.0)
    return train


def draw_train_points(key, part):
    return points_of(key).astype(jnp.bfloat16)


def draw_test_points(key, part):
    train = points_of(key)
    anchor = jax.random.randint(jax.random.fold_in(key, 12), (TEST,), 0, TRAIN)
    noise = jnp.clip(jax.random.normal(jax.random.fold_in(key, 13), (DIM, TEST), jnp.float32), -6.0, 6.0)
    spread = jnp.full((1, TEST), 0.5, jnp.float32)
    return (jnp.take(train, anchor, axis=1) + spread * noise).astype(jnp.bfloat16)


def draw_factor(key, part):
    base = jnp.clip(jax.random.normal(jax.random.fold_in(key, 21), (TRAIN, RANK), jnp.float32), -6.0, 6.0)
    return (base * (0.9 / math.sqrt(RANK))).astype(jnp.bfloat16)


def shard_levels(own_key, dims, pieces, low, high):
    def one(position, parts):
        steps = jax.random.uniform(jax.random.fold_in(jax.random.fold_in(own_key, 6), position), (parts,), jnp.float32, low / len(pieces), high / len(pieces))
        return jnp.repeat(jnp.exp(steps), dims[position] // parts).reshape((-1,) + (1,) * (len(dims) - position - 1))

    level = one(*pieces[0])
    for cut in pieces[1:]:
        level = level * one(*cut)
    return level


def normal_values(key, shape, scale, reach, split=(), kind=jnp.bfloat16):
    entries = jax.random.normal(key, shape, jnp.float32) * scale
    if len(split) > 0:
        entries = shard_levels(key, shape, split, -0.22, 0.18) * entries
    return jnp.clip(entries, min=-reach, max=reach).astype(kind)


def setup_inputs(seed: int = 0, part: int = 0) -> dict:
    streams_of = jax.random.split(jax.random.key(seed), 5)
    part_keys = jax.random.split(jax.random.fold_in(streams_of[4], part), 5)
    test_points = draw_test_points(jax.random.fold_in(jax.random.fold_in(streams_of[4], part), 71), part)
    train_points = draw_train_points(jax.random.fold_in(jax.random.fold_in(streams_of[4], part), 71), part)
    weights = normal_values(part_keys[2], (TRAIN,), 1.5, 6.0, ((0, 64),))
    factor = draw_factor(jax.random.fold_in(jax.random.fold_in(streams_of[4], part), 71), part)
    return dict(test_points=test_points, train_points=train_points, weights=weights, factor=factor)


def reference(test_points, train_points, weights, factor):
    test_sq = jnp.sum(test_points.astype(jnp.float32) ** 2, axis=0)
    total = train_points.shape[1]
    block = math.gcd(total, 1024)
    count = total // block
    width = factor.shape[1]
    rows = test_points.shape[1]

    def step(carry, index):
        mean_acc, proj_acc = carry
        start = (index * block).astype(jnp.int32)
        points = lax.dynamic_slice_in_dim(train_points, start, block, 1)
        wblock = lax.dynamic_slice_in_dim(weights, start, block, 0)
        fblock = lax.dynamic_slice_in_dim(factor, start, block, 0)
        train_sq = jnp.sum(points.astype(jnp.float32) ** 2, axis=0)
        cross = jnp.dot(test_points.T, points, preferred_element_type=jnp.float32)
        kernel = jnp.exp(-(test_sq[:, None] + train_sq[None, :] - 2.0 * cross) * (4.0 / DIM)).astype(jnp.bfloat16)
        mean_acc = mean_acc + jnp.dot(kernel, wblock, preferred_element_type=jnp.float32)
        proj_acc = proj_acc + jnp.dot(kernel, fblock, preferred_element_type=jnp.float32)
        return (mean_acc, proj_acc), None

    init = (jnp.zeros((rows,), jnp.float32), jnp.zeros((rows, width), jnp.float32))
    (mean, project), _ = lax.scan(step, init, jnp.arange(count, dtype=jnp.int32))
    variance = 1.0 - jnp.sum(project * project, axis=1)
    return mean, variance
```

```python
import functools
import math

import jax
import jax.numpy as jnp
from jax import lax
from jax.experimental import pallas as pl
from jax.experimental.pallas import tpu as pltpu
from jax.sharding import PartitionSpec as P

LOG2E = 1.4426950408889634
F32 = jnp.float32
BF16 = jnp.bfloat16
LANES = 128


def pieces_of(value):
    hi = value.astype(BF16).astype(F32)
    rest = value - hi
    mid = rest.astype(BF16).astype(F32)
    low = (rest - mid).astype(BF16).astype(F32)
    return hi, mid, low


def norm_rows(pieces, ones_first, width):
    row = lax.broadcasted_iota(jnp.int32, (16, width), 0)
    base = 3 if ones_first else 0
    ones = 0 if ones_first else 3
    block = jnp.where((row >= ones) & (row < ones + 3), F32(1), F32(0))
    for k, piece in enumerate(pieces):
        block = jnp.where(row == base + k, jnp.broadcast_to(piece, (16, width)), block)
    return block


def body(
    side, chunk,
    test_ref, train_ref, weight_ref, factor_hbm, mean_ref, var_ref,
    factor, lhs, rhs, send_r, send_l, recv_r, recv_l, part, msg, gather,
    load_sem, sr_sem, sl_sem, rr_sem, rl_sem, ps_sem, pr_sem, gs_sem, gr_sem,
):
    dim = test_ref.shape[0]
    local = train_ref.shape[1]
    rank = factor.shape[1]
    half = side // 2
    slots = side - 1
    me = lax.axis_index("trn")
    tst = lax.axis_index("tst")
    row_pos, col_pos = lax.div(me, side), lax.rem(me, side)
    pos1 = jnp.where(tst == 0, col_pos, row_pos)
    pos2 = jnp.where(tst == 0, row_pos, col_pos)
    stride1 = jnp.where(tst == 0, 1, side)
    stride2 = jnp.where(tst == 0, side, 1)

    def at(p1, p2):
        return p1 * stride1 + p2 * stride2

    right = at(lax.rem(pos1 + 1, side), pos2)
    left = at(lax.rem(pos1 + side - 1, side), pos2)

    step_rows = local // 4
    loads = []
    for c in range(4):
        rows = pl.ds(c * step_rows, step_rows)
        copy = pltpu.make_async_copy(factor_hbm.at[rows], factor.at[rows], load_sem.at[c])
        copy.start()
        loads.append(copy)
    barrier = pltpu.get_barrier_semaphore()
    for peer in (right, left):
        pl.semaphore_signal(barrier, inc=1, device_id={"trn": peer})
    for k in range(1, side):
        pl.semaphore_signal(barrier, inc=1, device_id={"trn": at(pos1, lax.rem(pos2 + k, side))})

    scale = 4.0 / dim
    train = train_ref[...].astype(F32)
    tsq = jnp.sum(train * train, axis=0, keepdims=True) * F32(-scale * LOG2E)
    parts = pieces_of(train * F32(2.0 * scale * LOG2E))
    for k in range(3):
        rhs[k * dim : (k + 1) * dim, :] = parts[k].astype(BF16)
    rhs[3 * dim : 3 * dim + 16, :] = norm_rows(pieces_of(tsq), False, local).astype(BF16)
    rhs[3 * dim + 16 :, :] = jnp.zeros((rhs.shape[0] - 3 * dim - 16, local), BF16)

    wide = 2 * LANES

    def turn(b, carry):
        cols = pl.ds(pl.multiple_of(b * wide, wide), wide)
        test = test_ref[:, cols].astype(F32)
        ssq = jnp.sum(test * test, axis=0, keepdims=True) * F32(-scale * LOG2E)
        rows = norm_rows(pieces_of(ssq), True, wide)
        pad = jnp.zeros((lhs.shape[1] - 3 * dim - 16, wide), F32)
        stack = jnp.concatenate([test, test, test, rows, pad], axis=0)
        lhs[cols, :] = stack.T.astype(BF16)
        return carry

    lax.fori_loop(0, test_ref.shape[1] // wide, turn, 0)
    for copy in loads:
        copy.wait()
    pl.semaphore_wait(barrier, 2 + side - 1)

    def copies(s):
        to_right = pltpu.make_async_remote_copy(
            src_ref=send_r.at[s], dst_ref=recv_r.at[s],
            send_sem=sr_sem.at[s], recv_sem=rr_sem.at[s], device_id={"trn": right},
        )
        to_left = pltpu.make_async_remote_copy(
            src_ref=send_l.at[s], dst_ref=recv_l.at[s],
            send_sem=sl_sem.at[s], recv_sem=rl_sem.at[s], device_id={"trn": left},
        )
        return to_right, to_left

    def slot(s, carry):
        distance = lax.div(side - s, 2)
        odd = lax.rem(s, 2)
        block_r = lax.rem(pos1 + distance, side)
        block_l = lax.rem(pos1 + side - distance, side)
        start_r = pl.multiple_of((block_r * 2 + odd) * LANES, LANES)
        start_l = pl.multiple_of((block_l * 2 + 1 - odd) * LANES, LANES)
        points = jnp.concatenate([lhs[pl.ds(start_r, LANES), :], lhs[pl.ds(start_l, LANES), :]], axis=0)
        total = jnp.zeros((wide, rank), F32)
        weighted = jnp.zeros((wide, LANES), F32)
        for c in range(local // chunk):
            cols = slice(c * chunk, (c + 1) * chunk)
            power = jnp.dot(points, rhs[:, cols], preferred_element_type=F32)
            kern = jnp.exp2(power).astype(BF16)
            total = total + jnp.dot(kern, factor[cols, :], preferred_element_type=F32)
            terms = kern.astype(F32) * weight_ref[:, cols].astype(F32)
            for g in range(chunk // LANES):
                weighted = weighted + terms[:, g * LANES : (g + 1) * LANES]
        for k, ref in enumerate((send_r, send_l)):
            rows = slice(k * LANES, (k + 1) * LANES)
            ref[s, :rank, :] = total[rows].T
            mean_row = jnp.sum(weighted[rows].T, axis=0, keepdims=True)
            ref[s, rank:, :] = jnp.broadcast_to(mean_row, (8, LANES))

        @pl.when(s >= 2)
        def _():
            to_right, to_left = copies(s - 2)
            to_right.wait_recv()
            to_left.wait_recv()
            send_r[s] = send_r[s] + recv_r[s - 2]
            send_l[s] = send_l[s] + recv_l[s - 2]

        @pl.when(s < slots)
        def _():
            to_right, to_left = copies(s)
            to_right.start()
            to_left.start()

        return carry

    lax.fori_loop(0, side, slot, 0)
    last_r, last_l = copies(slots - 1)
    last_r.wait_recv()
    last_l.wait_recv()
    send_l[slots] = send_l[slots] + recv_r[slots - 1]
    send_r[slots] = send_r[slots] + recv_l[slots - 1]

    share = rank // side
    sums = (send_l, send_r)

    def exchange(k, h):
        peer = lax.rem(pos2 + k, side)
        rows = pl.ds(pl.multiple_of(peer * share, share), share)
        return pltpu.make_async_remote_copy(
            src_ref=sums[h].at[slots, rows], dst_ref=part.at[k - 1, h],
            send_sem=ps_sem.at[k - 1, h], recv_sem=pr_sem.at[k - 1, h],
            device_id={"trn": at(pos1, peer)},
        )

    for k in range(1, side):
        for h in range(2):
            exchange(k, h).start()
    mine = pl.ds(pl.multiple_of(pos2 * share, share), share)
    squares = []
    for h in range(2):
        block = sums[h][slots, mine, :]
        for k in range(1, side):
            exchange(k, h).wait_recv()
            block = block + part[k - 1, h]
        squares.append(jnp.sum(block * block, axis=0, keepdims=True))
    line = lax.broadcasted_iota(jnp.int32, (4, LANES), 0)
    values = squares + [send_l[slots, rank : rank + 1, :], send_r[slots, rank : rank + 1, :]]
    packed = jnp.zeros((4, LANES), F32)
    for k, value in enumerate(values):
        packed = jnp.where(line == k, jnp.broadcast_to(value, (4, LANES)), packed)
    msg[...] = packed

    own = pos1 * side + pos2

    def spread(k):
        other = lax.rem(own + k, side * side)
        return pltpu.make_async_remote_copy(
            src_ref=msg, dst_ref=gather.at[own], send_sem=gs_sem, recv_sem=gr_sem,
            device_id={"trn": at(lax.div(other, side), lax.rem(other, side))},
        )

    def send(k, carry):
        spread(k).start()
        return carry

    lax.fori_loop(1, side * side, send, 0)
    gather[own] = packed

    def drain(s, carry):
        to_right, to_left = copies(s)
        to_right.wait_send()
        to_left.wait_send()
        return carry

    lax.fori_loop(0, slots, drain, 0)
    for k in range(1, side):
        for h in range(2):
            exchange(k, h).wait_send()
    others = gather.at[pl.ds(0, side * side - 1)]
    pltpu.make_async_remote_copy(
        src_ref=others, dst_ref=others, send_sem=gs_sem, recv_sem=gr_sem, device_id={"trn": right}
    ).wait()
    for p in range(side):
        total = gather[p * side]
        for q in range(1, side):
            total = total + gather[p * side + q]
        var_ref[p] = 1.0 - total[0:2]
        mean_ref[p] = total[2:4]


def on_device(side, test_points, train_points, weights, factor):
    dim, rows = test_points.shape
    local, rank = factor.shape
    slots = side - 1
    depth = 2 * LANES
    share = rank // side
    dma = pltpu.SemaphoreType.DMA
    vmem = pl.BlockSpec(memory_space=pltpu.VMEM)
    chunk_shape = (rank + 8, LANES)
    mean, var = pl.pallas_call(
        functools.partial(body, side, 1024),
        out_shape=[jax.ShapeDtypeStruct((side, 2, LANES), F32)] * 2,
        in_specs=[vmem, vmem, vmem, pl.BlockSpec(memory_space=pl.ANY)],
        out_specs=[vmem, vmem],
        scratch_shapes=[
            pltpu.VMEM((local, rank), BF16),
            pltpu.VMEM((rows, depth), BF16),
            pltpu.VMEM((depth, local), BF16),
            pltpu.VMEM((side, *chunk_shape), F32),
            pltpu.VMEM((side, *chunk_shape), F32),
            pltpu.VMEM((slots, *chunk_shape), F32),
            pltpu.VMEM((slots, *chunk_shape), F32),
            pltpu.VMEM((slots, 2, share, LANES), F32),
            pltpu.VMEM((4, LANES), F32),
            pltpu.VMEM((side * side, 4, LANES), F32),
            dma((4,)),
            dma((slots,)), dma((slots,)), dma((slots,)), dma((slots,)),
            dma((slots, 2)), dma((slots, 2)),
            dma, dma,
        ],
        compiler_params=pltpu.CompilerParams(
            collective_id=0, has_side_effects=True, vmem_limit_bytes=56 * 1024 * 1024
        ),
    )(test_points, train_points, weights.reshape(1, local), factor)
    return mean.reshape(rows), var.reshape(rows)


def solution(mesh):
    side = math.isqrt(mesh.shape["trn"])
    shared = ("grp", "trn")
    return jax.shard_map(
        functools.partial(on_device, side),
        mesh=mesh,
        in_specs=(P(None, ("grp", "tst")), P(None, shared), P(shared), P(shared, None)),
        out_specs=(P(("grp", "tst")), P(("grp", "tst"))),
        check_vma=False,
    )
```

```python
import functools
import math

import jax
import jax.numpy as jnp
from jax import lax
from jax.experimental import pallas as pl
from jax.experimental.pallas import tpu as pltpu
from jax.sharding import PartitionSpec as P

LOG2E = 1.4426950408889634
F32 = jnp.float32
BF16 = jnp.bfloat16
LANES = 128


def pieces_of(value):
    hi = value.astype(BF16).astype(F32)
    rest = value - hi
    mid = rest.astype(BF16).astype(F32)
    low = (rest - mid).astype(BF16).astype(F32)
    return hi, mid, low


def norm_rows(pieces, ones_first, width):
    row = lax.broadcasted_iota(jnp.int32, (16, width), 0)
    base = 3 if ones_first else 0
    ones = 0 if ones_first else 3
    block = jnp.where((row >= ones) & (row < ones + 3), F32(1), F32(0))
    for k, piece in enumerate(pieces):
        block = jnp.where(row == base + k, jnp.broadcast_to(piece, (16, width)), block)
    return block


def body(
    side, chunk,
    test_ref, train_ref, weight_ref, factor_hbm, out_ref,
    factor, lhs, rhs, part, recv, share_in, msg, gather,
    load_sem, s_sem, r_sem, ps_sem, pr_sem, gs_sem, gr_sem,
):
    dim = test_ref.shape[0]
    local = train_ref.shape[1]
    rank = factor.shape[1]
    half = side // 2
    slots = side - 1
    wide = 2 * LANES
    me = lax.axis_index("trn")
    row_pos, col_pos = lax.div(me, side), lax.rem(me, side)
    pos = (col_pos, row_pos)
    stride = (1, side)

    def moved(axis, k):
        there = lax.rem(pos[axis] + k + side, side)
        return me + (there - pos[axis]) * stride[axis]

    step_rows = local // 4
    loads = []
    for c in range(4):
        rows = pl.ds(c * step_rows, step_rows)
        copy = pltpu.make_async_copy(factor_hbm.at[rows], factor.at[rows], load_sem.at[c])
        copy.start()
        loads.append(copy)
    barrier = pltpu.get_barrier_semaphore()
    for axis in range(2):
        for k in range(1, side):
            pl.semaphore_signal(barrier, inc=1, device_id={"trn": moved(axis, k)})

    scale = 4.0 / dim
    train = train_ref[...].astype(F32)
    tsq = jnp.sum(train * train, axis=0, keepdims=True) * F32(-scale * LOG2E)
    parts = pieces_of(train * F32(2.0 * scale * LOG2E))
    for k in range(3):
        rhs[k * dim : (k + 1) * dim, :] = parts[k].astype(BF16)
    rhs[3 * dim : 3 * dim + 16, :] = norm_rows(pieces_of(tsq), False, local).astype(BF16)
    rhs[3 * dim + 16 :, :] = jnp.zeros((rhs.shape[0] - 3 * dim - 16, local), BF16)

    def turn(b, carry):
        cols = pl.ds(pl.multiple_of(b * wide, wide), wide)
        test = test_ref[:, cols].astype(F32)
        ssq = jnp.sum(test * test, axis=0, keepdims=True) * F32(-scale * LOG2E)
        rows = norm_rows(pieces_of(ssq), True, wide)
        pad = jnp.zeros((lhs.shape[1] - 3 * dim - 16, wide), F32)
        stack = jnp.concatenate([test, test, test, rows, pad], axis=0)
        lhs[cols, :] = stack.T.astype(BF16)
        return carry

    lax.fori_loop(0, test_ref.shape[1] // wide, turn, 0)
    for copy in loads:
        copy.wait()

    cut = rank // 2
    halves = (pl.ds(0, cut), pl.ds(cut, rank + 8 - cut))

    def place(way, distance):
        return distance if way == 0 or distance in (0, half) else half + distance

    def piece(way, s):
        return halves[(s + way) % 2]

    def hop(axis, way, s):
        rows = piece(way, s)
        return pltpu.make_async_remote_copy(
            src_ref=part.at[axis, place(way, (side - s) // 2), rows],
            dst_ref=recv.at[axis, way, s, pl.ds(0, rows.size)],
            send_sem=s_sem.at[axis, way, s], recv_sem=r_sem.at[axis, way, s],
            device_id={"trn": moved(axis, 1 if way == 0 else -1)},
        )

    def take(axis, way, s, distance):
        hop(axis, way, s).wait_recv()
        rows = piece(way, s)
        at = place(way, distance)
        part[axis, at, rows, :] = part[axis, at, rows, :] + recv[axis, way, s, : rows.size, :]

    def send(axis, s):
        for way in range(2):
            if s >= 2:
                take(axis, way, s - 2, (side - s) // 2)
            hop(axis, way, s).start()

    plan = {
        0: [(0, 0), (1, 0)],
        1: [(0, 1)],
        2: [(1, 1)],
        3: [(0, 2), (1, 2)],
        5: [(0, 3), (1, 3)],
        6: [(0, 4), (1, 4)],
        7: [(0, 5), (1, 5), (0, 6), (1, 6)],
    }

    def compute(i, carry):
        edge = (i == 0) | (i == side - 1)
        inner = lax.rem(i + 1, 2)
        distance = half - lax.div(i + 1, 2)
        distance = jnp.where(i == 0, half, jnp.where(i == side - 1, 0, distance))
        axes = (jnp.where(edge, 0, inner), jnp.where(edge, 1, inner))
        signed = (distance, jnp.where(edge, distance, -distance))
        places = (distance, jnp.where(edge, distance, half + distance))
        starts = []
        for k in range(2):
            at = jnp.where(axes[k] == 0, col_pos, row_pos)
            block = lax.rem(at + signed[k] + side, side)
            starts.append(pl.multiple_of((block * 2 + axes[k]) * LANES, LANES))
        points = jnp.concatenate([lhs[pl.ds(s, LANES), :] for s in starts], axis=0)
        total = jnp.zeros((wide, rank), F32)
        weighted = jnp.zeros((wide, LANES), F32)
        for c in range(local // chunk):
            cols = slice(c * chunk, (c + 1) * chunk)
            power = jnp.dot(points, rhs[:, cols], preferred_element_type=F32)
            kern = jnp.exp2(power).astype(BF16)
            total = total + jnp.dot(kern, factor[cols, :], preferred_element_type=F32)
            terms = kern.astype(F32) * weight_ref[cols].reshape(1, chunk).astype(F32)
            for g in range(chunk // LANES):
                weighted = weighted + terms[:, g * LANES : (g + 1) * LANES]
        for k in range(2):
            rows = slice(k * LANES, (k + 1) * LANES)
            part[axes[k], places[k], :rank, :] = total[rows].T
            mean_row = jnp.sum(weighted[rows].T, axis=0, keepdims=True)
            part[axes[k], places[k], rank:, :] = jnp.broadcast_to(mean_row, (8, LANES))

        for when, sends in plan.items():
            @pl.when(i == when)
            def _(when=when, sends=sends):
                if when == 0:
                    pl.semaphore_wait(barrier, 2 * slots)
                for axis, s in sends:
                    send(axis, s)

        return carry

    lax.fori_loop(0, side, compute, 0)

    share = rank // side
    order = sorted(range(1, side), key=lambda k: -min(k, side - k))

    def exchange(axis, k):
        peer = lax.rem(pos[1 - axis] + k, side)
        rows = pl.ds(pl.multiple_of(peer * share, share), share)
        return pltpu.make_async_remote_copy(
            src_ref=part.at[axis, 0, rows], dst_ref=share_in.at[axis, k - 1],
            send_sem=ps_sem.at[axis, k - 1], recv_sem=pr_sem.at[axis, k - 1],
            device_id={"trn": moved(1 - axis, k)},
        )

    for axis in range(2):
        for s in (slots - 2, slots - 1):
            for way in range(2):
                take(axis, way, s, 0)
        for k in order:
            exchange(axis, k).start()
    values = []
    for axis in range(2):
        mine = pl.ds(pl.multiple_of(pos[1 - axis] * share, share), share)
        block = part[axis, 0, mine, :]
        for k in range(1, side):
            exchange(axis, k).wait_recv()
            block = block + share_in[axis, k - 1]
        values.append(jnp.sum(block * block, axis=0, keepdims=True))
        values.append(part[axis, 0, rank : rank + 1, :])
    line = lax.broadcasted_iota(jnp.int32, (4, LANES), 0)
    packed = jnp.zeros((4, LANES), F32)
    for k, value in enumerate(values):
        packed = jnp.where(line == k, jnp.broadcast_to(value, (4, LANES)), packed)
    msg[...] = packed

    count = side * side

    def spread(j):
        k = lax.rem(j + count // 2 + half, count - 1) + 1
        other = lax.rem(me + k, count)
        return pltpu.make_async_remote_copy(
            src_ref=msg, dst_ref=gather.at[me], send_sem=gs_sem, recv_sem=gr_sem, device_id={"trn": other}
        )

    def tell(j, carry):
        spread(j).start()
        return carry

    lax.fori_loop(0, count - 1, tell, 0)
    gather[me] = packed
    for axis in range(2):
        for way in range(2):
            for s in range(slots):
                hop(axis, way, s).wait_send()
        for k in order:
            exchange(axis, k).wait_send()
    others = gather.at[pl.ds(0, count - 1)]
    pltpu.make_async_remote_copy(
        src_ref=others, dst_ref=others, send_sem=gs_sem, recv_sem=gr_sem, device_id={"trn": moved(0, 1)}
    ).wait()
    for p in range(side):
        for axis in range(2):
            total = jnp.zeros((4, LANES), F32)
            for q in range(side):
                total = total + gather[q * side + p if axis == 0 else p * side + q]
            row = 2 * p + axis
            out_ref[0, row : row + 1, :] = total[2 * axis : 2 * axis + 1]
            out_ref[1, row : row + 1, :] = -total[2 * axis + 1 : 2 * axis + 2]


def on_device(side, test_points, train_points, weights, factor):
    dim, rows = test_points.shape
    local, rank = factor.shape
    slots = side - 1
    depth = 2 * LANES
    share = rank // side
    dma = pltpu.SemaphoreType.DMA
    vmem = pl.BlockSpec(memory_space=pltpu.VMEM)
    out = pl.pallas_call(
        functools.partial(body, side, 1024),
        out_shape=jax.ShapeDtypeStruct((2, rows // LANES, LANES), F32),
        in_specs=[vmem, vmem, vmem, pl.BlockSpec(memory_space=pl.ANY)],
        out_specs=vmem,
        scratch_shapes=[
            pltpu.VMEM((local, rank), BF16),
            pltpu.VMEM((rows, depth), BF16),
            pltpu.VMEM((depth, local), BF16),
            pltpu.VMEM((2, side, rank + 8, LANES), F32),
            pltpu.VMEM((2, 2, slots, rank // 2 + 8, LANES), F32),
            pltpu.VMEM((2, slots, share, LANES), F32),
            pltpu.VMEM((4, LANES), F32),
            pltpu.VMEM((side * side, 4, LANES), F32),
            dma((4,)),
            dma((2, 2, slots)), dma((2, 2, slots)),
            dma((2, slots)), dma((2, slots)),
            dma, dma,
        ],
        compiler_params=pltpu.CompilerParams(
            collective_id=0, has_side_effects=True, vmem_limit_bytes=56 * 1024 * 1024
        ),
    )(test_points, train_points, weights, factor)
    return -out[1].reshape(rows), 1.0 - out[0].reshape(rows)


def solution(mesh):
    side = math.isqrt(mesh.shape["trn"])
    shared = ("grp", "trn")
    return jax.shard_map(
        functools.partial(on_device, side),
        mesh=mesh,
        in_specs=(P(None, ("grp", "tst")), P(None, shared), P(shared), P(shared, None)),
        out_specs=(P(("grp", "tst")), P(("grp", "tst"))),
        check_vma=False,
    )
```

```python
import functools
import math

import jax
import jax.numpy as jnp
from jax import lax
from jax.experimental import pallas as pl
from jax.experimental.pallas import tpu as pltpu
from jax.sharding import PartitionSpec as P

LOG2E = 1.4426950408889634
F32 = jnp.float32
BF16 = jnp.bfloat16
LANES = 128


def pieces_of(value):
    hi = value.astype(BF16).astype(F32)
    rest = value - hi
    mid = rest.astype(BF16).astype(F32)
    low = (rest - mid).astype(BF16).astype(F32)
    return hi, mid, low


def norm_rows(values, ones_first):
    width = values.shape[1]
    row = lax.broadcasted_iota(jnp.int32, (16, width), 0)
    base, ones = (3, 0) if ones_first else (0, 3)
    block = jnp.where((row >= ones) & (row < ones + 3), F32(1), F32(0))
    for k, piece in enumerate(pieces_of(values)):
        block = jnp.where(row == base + k, jnp.broadcast_to(piece, (16, width)), block)
    return block


def half_norms(points):
    points = points.astype(F32)
    return jnp.sum(points * points, axis=0, keepdims=True) * F32(-0.5)


def body(
    side, chunk,
    test_hbm, train_hbm, weight_hbm, factor_hbm, out_ref,
    test, train, weight, factor, lhs, rhs, part, recv, share_in, mean_own, mean_in, mean_all, msg, gather,
    load_sem, s_sem, r_sem, ps_sem, pr_sem, ms_sem, mr_sem, gs_sem, gr_sem, as_sem, ar_sem,
):
    dim, local = train.shape
    rank = factor.shape[1]
    half = side // 2
    slots = side - 1
    wide = 2 * LANES
    turns = local // chunk
    me = lax.axis_index("trn")
    row_pos, col_pos = lax.div(me, side), lax.rem(me, side)
    pos = (col_pos, row_pos)
    ring = [
        [lax.rem(pos[axis] + k, side) * (1, side)[axis] for k in range(side)] for axis in range(2)
    ]

    def moved(axis, k):
        k = k % side
        return ring[0][k] + ring[1][0] if axis == 0 else ring[0][0] + ring[1][k]

    def load(k, src, dst):
        copy = pltpu.make_async_copy(src, dst, load_sem.at[k])
        copy.start()
        return copy

    get_test = load(0, test_hbm, test)
    get_train = load(1, train_hbm, train)
    get_weight = load(2, weight_hbm, weight)
    get_factor = []
    for c in range(turns):
        rows = pl.ds(c * chunk, chunk)
        get_factor.append(load(3 + c, factor_hbm.at[rows], factor.at[rows]))
    barrier = pltpu.get_barrier_semaphore()
    for axis in range(2):
        for k in range(1, side):
            pl.semaphore_signal(barrier, inc=1, device_id={"trn": moved(axis, k)})

    pad = jnp.zeros((LANES - dim - 16, LANES), F32)
    get_test.wait()
    for b in range(test.shape[1] // LANES):
        cols = slice(b * LANES, (b + 1) * LANES)
        points = test[:, cols].astype(F32)
        stack = jnp.concatenate([points, norm_rows(half_norms(points), True), pad], axis=0)
        lhs[cols, :] = stack.T.astype(BF16)
    get_train.wait()
    rhs[dim + 16 :, :] = jnp.zeros((LANES - dim - 16, local), BF16)
    for c in range(turns):
        cols = slice(c * chunk, (c + 1) * chunk)
        points = train[:, cols]
        rhs[:dim, cols] = points
        rhs[dim : dim + 16, cols] = norm_rows(half_norms(points), False).astype(BF16)
    get_weight.wait()

    cut = rank // 2
    halves = (pl.ds(0, cut), pl.ds(cut, rank + 8 - cut))

    def place(way, distance):
        return distance if way == 0 or distance in (0, half) else half + distance

    def piece(way, s):
        return halves[(s + way) % 2]

    def hop(axis, way, s):
        rows = piece(way, s)
        return pltpu.make_async_remote_copy(
            src_ref=part.at[axis, place(way, (side - s) // 2), rows],
            dst_ref=recv.at[axis, way, s, pl.ds(0, rows.size)],
            send_sem=s_sem.at[axis, way, s], recv_sem=r_sem.at[axis, way, s],
            device_id={"trn": moved(axis, 1 if way == 0 else -1)},
        )

    def take(axis, way, s, distance):
        hop(axis, way, s).wait_recv()
        rows = piece(way, s)
        at = place(way, distance)
        part[axis, at, rows, :] = part[axis, at, rows, :] + recv[axis, way, s, : rows.size, :]

    def send(axis, s):
        for way in range(2):
            if s >= 2:
                take(axis, way, s - 2, (side - s) // 2)
            hop(axis, way, s).start()

    def compute(starts, axes, places, first):
        points = jnp.concatenate([lhs[pl.ds(s, LANES), :] for s in starts], axis=0)
        total = jnp.zeros((wide, rank), F32)
        weighted = jnp.zeros((wide, LANES), F32)
        for c in range(turns):
            cols = slice(c * chunk, (c + 1) * chunk)
            power = jnp.dot(points, rhs[:, cols], preferred_element_type=F32)
            kern = jnp.exp2(power * F32(8.0 / dim * LOG2E)).astype(BF16)
            if first:
                get_factor[c].wait()
            total = total + jnp.dot(kern, factor[cols, :], preferred_element_type=F32)
            terms = kern.astype(F32) * weight[cols].reshape(1, chunk).astype(F32)
            for g in range(chunk // LANES):
                weighted = weighted + terms[:, g * LANES : (g + 1) * LANES]
        for k in range(2):
            rows = slice(k * LANES, (k + 1) * LANES)
            part[axes[k], places[k], :rank, :] = total[rows].T
            mean_row = jnp.sum(weighted[rows].T, axis=0, keepdims=True)
            part[axes[k], places[k], rank:, :] = jnp.broadcast_to(mean_row, (8, LANES))

    def start_of(axis, distance):
        at = col_pos if isinstance(axis, int) and axis == 0 else row_pos
        if not isinstance(axis, int):
            at = jnp.where(axis == 0, col_pos, row_pos)
        block = lax.rem(at + distance + side, side)
        return pl.multiple_of((block * 2 + axis) * LANES, LANES)

    compute([start_of(0, half), start_of(1, half)], (0, 1), (half, half), True)
    pl.semaphore_wait(barrier, 2 * slots)
    send(0, 0)
    send(1, 0)

    plan = {
        1: [(0, 1)],
        2: [(1, 1)],
        3: [(0, 2), (1, 2)],
        4: [(0, 3), (1, 3)],
        5: [(0, 4), (1, 4)],
        6: [(0, 5), (1, 5), (0, 6), (1, 6)],
    }

    def step(i, carry):
        last = i == slots
        inner = lax.rem(i + 1, 2)
        distance = jnp.where(last, 0, half - lax.div(i + 1, 2))
        axes = (jnp.where(last, 0, inner), jnp.where(last, 1, inner))
        places = (distance, jnp.where(last, 0, half + distance))
        compute([start_of(axes[0], distance), start_of(axes[1], -distance)], axes, places, False)
        for when, sends in plan.items():
            @pl.when(i == when)
            def _(sends=sends):
                for axis, s in sends:
                    send(axis, s)

        return carry

    lax.fori_loop(1, side, step, 0)

    share = rank // side
    order = sorted(range(1, side), key=lambda k: -min(k, side - k))

    def exchange(axis, k):
        peer = lax.rem(pos[1 - axis] + k, side)
        rows = pl.ds(pl.multiple_of(peer * share, share), share)
        return pltpu.make_async_remote_copy(
            src_ref=part.at[axis, 0, rows], dst_ref=share_in.at[axis, k - 1],
            send_sem=ps_sem.at[axis, k - 1], recv_sem=pr_sem.at[axis, k - 1],
            device_id={"trn": moved(1 - axis, k)},
        )

    def add_mean(axis, k):
        return pltpu.make_async_remote_copy(
            src_ref=mean_own.at[axis], dst_ref=mean_in.at[axis, k - 1],
            send_sem=ms_sem, recv_sem=mr_sem, device_id={"trn": moved(1 - axis, k)},
        )

    for axis in range(2):
        for s in (slots - 2, slots - 1):
            for way in range(2):
                take(axis, way, s, 0)
        mean_own[axis] = part[axis, 0, rank : rank + 1, :]
        for k in order:
            exchange(axis, k).start()
            add_mean(axis, k).start()
    for axis in range(2):
        mine = pl.ds(pl.multiple_of(pos[1 - axis] * share, share), share)
        block = part[axis, 0, mine, :]
        for k in order[::-1]:
            exchange(axis, k).wait_recv()
            block = block + share_in[axis, k - 1]
        msg[axis : axis + 1, :] = jnp.sum(block * block, axis=0, keepdims=True)

    far = lambda k: min(k, side - k)
    others = [(kx, ky) for kx in range(side) for ky in range(side) if (kx, ky) != (0, 0)]

    def spread(kx, ky):
        return pltpu.make_async_remote_copy(
            src_ref=msg, dst_ref=gather.at[me], send_sem=gs_sem, recv_sem=gr_sem,
            device_id={"trn": ring[0][kx] + ring[1][ky]},
        )

    for kx, ky in sorted(others, key=lambda k: -far(k[0]) - far(k[1])):
        spread(kx, ky).start()
    gather[me] = msg[...]

    def all_of(ref, send_sem, recv_sem):
        return pltpu.make_async_remote_copy(
            src_ref=ref, dst_ref=ref, send_sem=send_sem, recv_sem=recv_sem, device_id={"trn": moved(0, 1)}
        )

    all_of(mean_in, ms_sem, mr_sem).wait()
    for axis in range(2):
        mean = mean_own[axis]
        for k in range(1, side):
            mean = mean + mean_in[axis, k - 1]
        mean_all[axis, pos[axis]] = mean

    def tell(axis, k):
        return pltpu.make_async_remote_copy(
            src_ref=mean_all.at[axis, pos[axis]], dst_ref=mean_all.at[axis, pos[axis]],
            send_sem=as_sem, recv_sem=ar_sem, device_id={"trn": moved(axis, k)},
        )

    for axis in range(2):
        for k in order:
            tell(axis, k).start()
    for axis in range(2):
        for way in range(2):
            for s in range(slots):
                hop(axis, way, s).wait_send()
        for k in order:
            exchange(axis, k).wait_send()
    all_of(mean_all.at[:, pl.ds(0, slots)], as_sem, ar_sem).wait()
    all_of(gather.at[pl.ds(0, side * side - 1)], gs_sem, gr_sem).wait()
    for p in range(side):
        for axis in range(2):
            total = jnp.zeros((2, LANES), F32)
            for q in range(side):
                total = total + gather[q * side + p if axis == 0 else p * side + q]
            row = 2 * p + axis
            out_ref[0, row : row + 1, :] = total[axis : axis + 1]
            out_ref[1, row : row + 1, :] = -mean_all[axis, p]


def on_device(side, test_points, train_points, weights, factor):
    dim, rows = test_points.shape
    local, rank = factor.shape
    slots = side - 1
    share = rank // side
    chunk = 1024
    dma = pltpu.SemaphoreType.DMA
    out = pl.pallas_call(
        functools.partial(body, side, chunk),
        out_shape=jax.ShapeDtypeStruct((2, rows // LANES, LANES), F32),
        in_specs=[pl.BlockSpec(memory_space=pl.ANY)] * 4,
        out_specs=pl.BlockSpec(memory_space=pltpu.VMEM),
        scratch_shapes=[
            pltpu.VMEM((dim, rows), BF16),
            pltpu.VMEM((dim, local), BF16),
            pltpu.VMEM((local,), BF16),
            pltpu.VMEM((local, rank), BF16),
            pltpu.VMEM((rows, LANES), BF16),
            pltpu.VMEM((LANES, local), BF16),
            pltpu.VMEM((2, side, rank + 8, LANES), F32),
            pltpu.VMEM((2, 2, slots, rank // 2 + 8, LANES), F32),
            pltpu.VMEM((2, slots, share, LANES), F32),
            pltpu.VMEM((2, 1, LANES), F32),
            pltpu.VMEM((2, slots, 1, LANES), F32),
            pltpu.VMEM((2, side, 1, LANES), F32),
            pltpu.VMEM((2, LANES), F32),
            pltpu.VMEM((side * side, 2, LANES), F32),
            dma((3 + local // chunk,)),
            dma((2, 2, slots)), dma((2, 2, slots)),
            dma((2, slots)), dma((2, slots)),
            dma, dma, dma, dma, dma, dma,
        ],
        compiler_params=pltpu.CompilerParams(
            collective_id=0, has_side_effects=True, vmem_limit_bytes=56 * 1024 * 1024
        ),
    )(test_points, train_points, weights, factor)
    return -out[1].reshape(rows), 1.0 - out[0].reshape(rows)


def solution(mesh):
    side = math.isqrt(mesh.shape["trn"])
    shared = ("grp", "trn")
    return jax.shard_map(
        functools.partial(on_device, side),
        mesh=mesh,
        in_specs=(P(None, ("grp", "tst")), P(None, shared), P(shared), P(shared, None)),
        out_specs=(P(("grp", "tst")), P(("grp", "tst"))),
        check_vma=False,
    )
```

```python
import functools
import math

import jax
import jax.numpy as jnp
from jax import lax
from jax.experimental import pallas as pl
from jax.experimental.pallas import tpu as pltpu
from jax.sharding import PartitionSpec as P

LOG2E = 1.4426950408889634
F32 = jnp.float32
BF16 = jnp.bfloat16
LANES = 128


def pieces_of(value):
    hi = value.astype(BF16).astype(F32)
    rest = value - hi
    mid = rest.astype(BF16).astype(F32)
    low = (rest - mid).astype(BF16).astype(F32)
    return hi, mid, low


def norm_rows(values, ones_first):
    width = values.shape[1]
    row = lax.broadcasted_iota(jnp.int32, (16, width), 0)
    base, ones = (3, 0) if ones_first else (0, 3)
    block = jnp.where((row >= ones) & (row < ones + 3), F32(1), F32(0))
    for k, piece in enumerate(pieces_of(values)):
        block = jnp.where(row == base + k, jnp.broadcast_to(piece, (16, width)), block)
    return block


def half_norms(points):
    points = points.astype(F32)
    return jnp.sum(points * points, axis=0, keepdims=True) * F32(-0.5)


def body(
    side, chunk,
    test_hbm, train_hbm, weight_hbm, factor_hbm, out_ref,
    test, train, weight, factor, lhs, rhs, part, recv, share_in, mean_own, mean_in, mean_all, msg, gather,
    load_sem, s_sem, r_sem, ps_sem, pr_sem, ms_sem, mr_sem, gs_sem, gr_sem, as_sem, ar_sem,
):
    dim, local = train.shape
    rank = factor.shape[1]
    half = side // 2
    slots = side - 1
    wide = 2 * LANES
    turns = local // chunk
    me = lax.axis_index("trn")
    row_pos, col_pos = lax.div(me, side), lax.rem(me, side)
    pos = (col_pos, row_pos)
    ring = [
        [lax.rem(pos[axis] + k, side) * (1, side)[axis] for k in range(side)] for axis in range(2)
    ]

    def moved(axis, k):
        k = k % side
        return ring[0][k] + ring[1][0] if axis == 0 else ring[0][0] + ring[1][k]

    def load(k, src, dst):
        copy = pltpu.make_async_copy(src, dst, load_sem.at[k])
        copy.start()
        return copy

    get_test = load(0, test_hbm, test)
    get_train = load(1, train_hbm, train)
    get_weight = load(2, weight_hbm, weight)
    barrier = pltpu.get_barrier_semaphore()
    for axis in range(2):
        for k in (1, -1):
            pl.semaphore_signal(barrier, inc=1, device_id={"trn": moved(axis, k)})

    pad = jnp.zeros((LANES - dim - 16, LANES), F32)
    get_test.wait()
    get_factor = []
    for c in range(turns):
        rows = pl.ds(c * chunk, chunk)
        get_factor.append(load(3 + c, factor_hbm.at[rows], factor.at[rows]))
    for b in range(test.shape[1] // LANES):
        cols = slice(b * LANES, (b + 1) * LANES)
        points = test[:, cols].astype(F32)
        stack = jnp.concatenate([points, norm_rows(half_norms(points), True), pad], axis=0)
        lhs[cols, :] = stack.T.astype(BF16)
    get_train.wait()
    get_weight.wait()

    quarter = rank // 4
    ends = [quarter * g for g in range(4)] + [rank + 1]
    quarters = [pl.ds(ends[g], ends[g + 1] - ends[g]) for g in range(4)]

    def place(way, distance):
        return distance if way == 0 or distance in (0, half) else half + distance

    def piece(way, s, j):
        return quarters[2 * ((s + way) % 2) + j]

    def hop(axis, way, s, j):
        rows = piece(way, s, j)
        return pltpu.make_async_remote_copy(
            src_ref=part.at[axis, place(way, (side - s) // 2), rows],
            dst_ref=recv.at[axis, way, s, j, pl.ds(0, rows.size)],
            send_sem=s_sem.at[axis, way, s, j], recv_sem=r_sem.at[axis, way, s, j],
            device_id={"trn": moved(axis, 1 if way == 0 else -1)},
        )

    def take(axis, way, s, distance, j):
        hop(axis, way, s, j).wait_recv()
        rows = piece(way, s, j)
        at = place(way, distance)
        part[axis, at, rows, :] = part[axis, at, rows, :] + recv[axis, way, s, j, : rows.size, :]

    def send(sends):
        for j in range(2):
            for axis, s in sends:
                for way in range(2):
                    if s >= 2:
                        take(axis, way, s - 2, (side - s) // 2, j)
                    hop(axis, way, s, j).start()

    def compute(starts, axes, places, first):
        points = jnp.concatenate([lhs[pl.ds(s, LANES), :] for s in starts], axis=0)
        total = jnp.zeros((wide, rank), F32)
        weighted = jnp.zeros((wide, LANES), F32)
        kerns = []
        for c in range(turns):
            cols = slice(c * chunk, (c + 1) * chunk)
            if first:
                rhs[:dim, cols] = train[:, cols]
                rhs[dim : dim + 16, cols] = norm_rows(half_norms(train[:, cols]), False).astype(BF16)
                rhs[dim + 16 :, cols] = jnp.zeros((LANES - dim - 16, chunk), BF16)
            power = jnp.dot(points, rhs[:, cols], preferred_element_type=F32)
            kern = jnp.exp2(power * F32(8.0 / dim * LOG2E)).astype(BF16)
            terms = kern.astype(F32) * weight[cols].reshape(1, chunk).astype(F32)
            for g in range(chunk // LANES):
                weighted = weighted + terms[:, g * LANES : (g + 1) * LANES]
            if first:
                kerns.append(kern)
            else:
                total = total + jnp.dot(kern, factor[cols, :], preferred_element_type=F32)
        for c, kern in enumerate(kerns):
            get_factor[c].wait()
            total = total + jnp.dot(kern, factor[c * chunk : (c + 1) * chunk, :], preferred_element_type=F32)
        for k in range(2):
            rows = slice(k * LANES, (k + 1) * LANES)
            part[axes[k], places[k], :rank, :] = total[rows].T
            mean_row = jnp.sum(weighted[rows].T, axis=0, keepdims=True)
            part[axes[k], places[k], rank:, :] = jnp.broadcast_to(mean_row, (8, LANES))

    def start_of(axis, distance):
        at = col_pos if isinstance(axis, int) and axis == 0 else row_pos
        if not isinstance(axis, int):
            at = jnp.where(axis == 0, col_pos, row_pos)
        block = lax.rem(at + distance + side, side)
        return pl.multiple_of((block * 2 + axis) * LANES, LANES)

    compute([start_of(0, half), start_of(1, half)], (0, 1), (half, half), True)
    pl.semaphore_wait(barrier, 4)
    plan = [
        (0, [(0, 0), (1, 0)]),
        (1, [(0, 1)]),
        (2, [(1, 1)]),
        (3, [(0, 2), (1, 2)]),
        (4, [(0, 3), (1, 3)]),
        (5, [(0, 4), (1, 4)]),
        (6, [(0, 5), (1, 5)]),
        (6, [(0, 6), (1, 6)]),
    ]

    def events(i):
        for when, sends in plan:
            if when == 0:
                continue

            @pl.when(i == when)
            def _(sends=sends):
                send(sends)

    send(plan[0][1])

    def step(i, carry):
        last = i == slots
        inner = lax.rem(i + 1, 2)
        distance = jnp.where(last, 0, half - lax.div(i + 1, 2))
        axes = (jnp.where(last, 0, inner), jnp.where(last, 1, inner))
        places = (distance, jnp.where(last, 0, half + distance))
        compute([start_of(axes[0], distance), start_of(axes[1], -distance)], axes, places, False)
        events(i)
        return carry

    lax.fori_loop(1, side, step, 0)

    share = quarter // side
    order = sorted(range(1, side), key=lambda k: -min(k, side - k))

    def exchange(axis, g, k):
        peer = lax.rem(pos[1 - axis] + k, side)
        rows = pl.ds(pl.multiple_of(quarter * g + peer * share, share), share)
        return pltpu.make_async_remote_copy(
            src_ref=part.at[axis, 0, rows], dst_ref=share_in.at[axis, g, k - 1],
            send_sem=ps_sem.at[axis, g], recv_sem=pr_sem.at[axis, g],
            device_id={"trn": moved(1 - axis, k)},
        )

    def add_mean(axis, k):
        return pltpu.make_async_remote_copy(
            src_ref=mean_own.at[axis], dst_ref=mean_in.at[axis, k - 1],
            send_sem=ms_sem, recv_sem=mr_sem, device_id={"trn": moved(1 - axis, k)},
        )

    def all_of(ref, send_sem, recv_sem):
        return pltpu.make_async_remote_copy(
            src_ref=ref, dst_ref=ref, send_sem=send_sem, recv_sem=recv_sem, device_id={"trn": moved(0, 1)}
        )

    for j in range(2):
        for axis in range(2):
            for way in range(2):
                take(axis, way, slots - 2, 0, j)
    for j in range(2):
        for axis in range(2):
            for way in range(2):
                take(axis, way, slots - 1, 0, j)
                for k in order:
                    exchange(axis, 2 * ((slots - 1 + way) % 2) + j, k).start()
    for axis in range(2):
        mean_own[axis] = part[axis, 0, rank : rank + 1, :]
        for k in order:
            add_mean(axis, k).start()
    for axis in range(2):
        total = jnp.zeros((1, LANES), F32)
        for g in (0, 2, 1, 3):
            all_of(share_in.at[axis, g], ps_sem.at[axis, g], pr_sem.at[axis, g]).wait_recv()
            block = part[axis, 0, pl.ds(pl.multiple_of(quarter * g + pos[1 - axis] * share, share), share), :]
            for k in range(slots):
                block = block + share_in[axis, g, k]
            total = total + jnp.sum(block * block, axis=0, keepdims=True)
        msg[axis : axis + 1, :] = total

    far = lambda k: min(k, side - k)
    others = [(kx, ky) for kx in range(side) for ky in range(side) if (kx, ky) != (0, 0)]

    def spread(kx, ky):
        return pltpu.make_async_remote_copy(
            src_ref=msg, dst_ref=gather.at[me], send_sem=gs_sem, recv_sem=gr_sem,
            device_id={"trn": ring[0][kx] + ring[1][ky]},
        )

    for kx, ky in sorted(others, key=lambda k: -far(k[0]) - far(k[1])):
        spread(kx, ky).start()
    gather[me] = msg[...]

    all_of(mean_in, ms_sem, mr_sem).wait()
    for axis in range(2):
        mean = mean_own[axis]
        for k in range(1, side):
            mean = mean + mean_in[axis, k - 1]
        mean_all[axis, pos[axis]] = mean

    def tell(axis, k):
        return pltpu.make_async_remote_copy(
            src_ref=mean_all.at[axis, pos[axis]], dst_ref=mean_all.at[axis, pos[axis]],
            send_sem=as_sem, recv_sem=ar_sem, device_id={"trn": moved(axis, k)},
        )

    for axis in range(2):
        for k in order:
            tell(axis, k).start()
    for axis in range(2):
        for way in range(2):
            for s in range(slots):
                for j in range(2):
                    hop(axis, way, s, j).wait_send()
        for g in range(4):
            all_of(share_in.at[axis, g], ps_sem.at[axis, g], pr_sem.at[axis, g]).wait_send()
    all_of(mean_all.at[:, pl.ds(0, slots)], as_sem, ar_sem).wait()
    all_of(gather.at[pl.ds(0, side * side - 1)], gs_sem, gr_sem).wait()
    for p in range(side):
        for axis in range(2):
            total = jnp.zeros((2, LANES), F32)
            for q in range(side):
                total = total + gather[q * side + p if axis == 0 else p * side + q]
            row = 2 * p + axis
            out_ref[0, row : row + 1, :] = total[axis : axis + 1]
            out_ref[1, row : row + 1, :] = -mean_all[axis, p]


def on_device(side, test_points, train_points, weights, factor):
    dim, rows = test_points.shape
    local, rank = factor.shape
    slots = side - 1
    share = rank // 4 // side
    chunk = 1024
    dma = pltpu.SemaphoreType.DMA
    out = pl.pallas_call(
        functools.partial(body, side, chunk),
        out_shape=jax.ShapeDtypeStruct((2, rows // LANES, LANES), F32),
        in_specs=[pl.BlockSpec(memory_space=pl.ANY)] * 4,
        out_specs=pl.BlockSpec(memory_space=pltpu.VMEM),
        scratch_shapes=[
            pltpu.VMEM((dim, rows), BF16),
            pltpu.VMEM((dim, local), BF16),
            pltpu.VMEM((local,), BF16),
            pltpu.VMEM((local, rank), BF16),
            pltpu.VMEM((rows, LANES), BF16),
            pltpu.VMEM((LANES, local), BF16),
            pltpu.VMEM((2, side, rank + 8, LANES), F32),
            pltpu.VMEM((2, 2, slots, 2, rank // 4 + 8, LANES), F32),
            pltpu.VMEM((2, 4, slots, share, LANES), F32),
            pltpu.VMEM((2, 1, LANES), F32),
            pltpu.VMEM((2, slots, 1, LANES), F32),
            pltpu.VMEM((2, side, 1, LANES), F32),
            pltpu.VMEM((2, LANES), F32),
            pltpu.VMEM((side * side, 2, LANES), F32),
            dma((3 + local // chunk,)),
            dma((2, 2, slots, 2)), dma((2, 2, slots, 2)),
            dma((2, 4)), dma((2, 4)),
            dma, dma, dma, dma, dma, dma,
        ],
        compiler_params=pltpu.CompilerParams(
            collective_id=0, has_side_effects=True, vmem_limit_bytes=40 * 1024 * 1024
        ),
    )(*(pltpu.with_memory_space_constraint(x, pltpu.HBM) for x in (test_points, train_points, weights, factor)))
    return -out[1].reshape(rows), 1.0 - out[0].reshape(rows)


def solution(mesh):
    side = math.isqrt(mesh.shape["trn"])
    shared = ("grp", "trn")
    return jax.shard_map(
        functools.partial(on_device, side),
        mesh=mesh,
        in_specs=(P(None, ("grp", "tst")), P(None, shared), P(shared), P(shared, None)),
        out_specs=(P(("grp", "tst")), P(("grp", "tst"))),
        check_vma=False,
    )
```

```python
import functools
import math

import jax
import jax.numpy as jnp
from jax import lax
from jax.experimental import pallas as pl
from jax.experimental.pallas import tpu as pltpu
from jax.sharding import PartitionSpec as P

LOG2E = 1.4426950408889634
F32 = jnp.float32
BF16 = jnp.bfloat16
LANES = 128


def pieces_of(value):
    hi = value.astype(BF16).astype(F32)
    rest = value - hi
    mid = rest.astype(BF16).astype(F32)
    low = (rest - mid).astype(BF16).astype(F32)
    return hi, mid, low


def norm_rows(values, ones_first):
    width = values.shape[1]
    row = lax.broadcasted_iota(jnp.int32, (16, width), 0)
    base, ones = (3, 0) if ones_first else (0, 3)
    block = jnp.where((row >= ones) & (row < ones + 3), F32(1), F32(0))
    for k, piece in enumerate(pieces_of(values)):
        block = jnp.where(row == base + k, jnp.broadcast_to(piece, (16, width)), block)
    return block


def half_norms(points):
    points = points.astype(F32)
    return jnp.sum(points * points, axis=0, keepdims=True) * F32(-0.5)


def body(
    side, chunk,
    test_hbm, train_hbm, weight_hbm, factor_hbm, out_ref,
    test, train, weight, factor, lhs, rhs, part, recv, share_in, mean_own, mean_in, mean_all, msg, gather,
    load_sem, s_sem, r_sem, ps_sem, pr_sem, ms_sem, mr_sem, gs_sem, gr_sem, as_sem, ar_sem,
):
    dim, local = train.shape
    rank = factor.shape[1]
    half = side // 2
    slots = side - 1
    wide = 2 * LANES
    turns = local // chunk
    me = lax.axis_index("trn")
    row_pos, col_pos = lax.div(me, side), lax.rem(me, side)
    pos = (col_pos, row_pos)
    ring = [
        [lax.rem(pos[axis] + k, side) * (1, side)[axis] for k in range(side)] for axis in range(2)
    ]

    def moved(axis, k):
        k = k % side
        return ring[0][k] + ring[1][0] if axis == 0 else ring[0][0] + ring[1][k]

    def load(k, src, dst):
        copy = pltpu.make_async_copy(src, dst, load_sem.at[k])
        copy.start()
        return copy

    get_test = load(0, test_hbm, test)
    get_train = load(1, train_hbm, train)
    get_weight = load(2, weight_hbm, weight)

    def load_factor(c):
        rows = pl.ds(c * chunk, chunk)
        return load(3 + c, factor_hbm.at[rows], factor.at[rows])

    get_factor = [load_factor(0)]
    barrier = pltpu.get_barrier_semaphore()
    for axis in range(2):
        for k in (1, -1):
            pl.semaphore_signal(barrier, inc=1, device_id={"trn": moved(axis, k)})

    pad = jnp.zeros((LANES - dim - 16, LANES), F32)
    get_test.wait()
    get_factor += [load_factor(c) for c in range(1, turns)]
    for b in range(test.shape[1] // LANES):
        cols = slice(b * LANES, (b + 1) * LANES)
        points = test[:, cols].astype(F32)
        stack = jnp.concatenate([points, norm_rows(half_norms(points), True), pad], axis=0)
        lhs[cols, :] = stack.T.astype(BF16)
    get_train.wait()
    get_weight.wait()

    quarter = rank // 4
    ends = [quarter * g for g in range(4)] + [rank + 1]
    quarters = [pl.ds(ends[g], ends[g + 1] - ends[g]) for g in range(4)]

    def place(way, distance):
        return distance if way == 0 or distance in (0, half) else half + distance

    def piece(way, s, j):
        return quarters[2 * ((s + way) % 2) + j]

    def hop(axis, way, s, j):
        rows = piece(way, s, j)
        return pltpu.make_async_remote_copy(
            src_ref=part.at[axis, place(way, (side - s) // 2), rows],
            dst_ref=recv.at[axis, way, s, j, pl.ds(0, rows.size)],
            send_sem=s_sem.at[axis, way, s, j], recv_sem=r_sem.at[axis, way, s, j],
            device_id={"trn": moved(axis, 1 if way == 0 else -1)},
        )

    def take(axis, way, s, distance, j):
        hop(axis, way, s, j).wait_recv()
        rows = piece(way, s, j)
        at = place(way, distance)
        part[axis, at, rows, :] = part[axis, at, rows, :] + recv[axis, way, s, j, : rows.size, :]

    def send(sends):
        for j in range(2):
            for axis, s in sends:
                for way in range(2):
                    if s >= 2:
                        take(axis, way, s - 2, (side - s) // 2, j)
                    hop(axis, way, s, j).start()

    def compute(starts, axes, places, first):
        points = jnp.concatenate([lhs[pl.ds(s, LANES), :] for s in starts], axis=0)
        total = jnp.zeros((wide, rank), F32)
        weighted = jnp.zeros((wide, LANES), F32)
        kerns = []
        for c in range(turns):
            cols = slice(c * chunk, (c + 1) * chunk)
            if first:
                rhs[:dim, cols] = train[:, cols]
                rhs[dim : dim + 16, cols] = norm_rows(half_norms(train[:, cols]), False).astype(BF16)
                rhs[dim + 16 :, cols] = jnp.zeros((LANES - dim - 16, chunk), BF16)
            power = jnp.dot(points, rhs[:, cols], preferred_element_type=F32)
            kern = jnp.exp2(power * F32(8.0 / dim * LOG2E)).astype(BF16)
            terms = kern.astype(F32) * weight[cols].reshape(1, chunk).astype(F32)
            for g in range(chunk // LANES):
                weighted = weighted + terms[:, g * LANES : (g + 1) * LANES]
            if first:
                kerns.append(kern)
            else:
                total = total + jnp.dot(kern, factor[cols, :], preferred_element_type=F32)
        for c, kern in enumerate(kerns):
            get_factor[c].wait()
            total = total + jnp.dot(kern, factor[c * chunk : (c + 1) * chunk, :], preferred_element_type=F32)
        for k in range(2):
            rows = slice(k * LANES, (k + 1) * LANES)
            part[axes[k], places[k], :rank, :] = total[rows].T
            mean_row = jnp.sum(weighted[rows].T, axis=0, keepdims=True)
            part[axes[k], places[k], rank:, :] = jnp.broadcast_to(mean_row, (8, LANES))

    def start_of(axis, distance):
        at = col_pos if isinstance(axis, int) and axis == 0 else row_pos
        if not isinstance(axis, int):
            at = jnp.where(axis == 0, col_pos, row_pos)
        block = lax.rem(at + distance + side, side)
        return pl.multiple_of((block * 2 + axis) * LANES, LANES)

    compute([start_of(0, half), start_of(1, half)], (0, 1), (half, half), True)
    pl.semaphore_wait(barrier, 4)
    plan = [
        (0, [(0, 0), (1, 0)]),
        (1, [(0, 1)]),
        (2, [(1, 1)]),
        (3, [(0, 2), (1, 2)]),
        (4, [(0, 3), (1, 3)]),
        (5, [(0, 4), (1, 4)]),
        (6, [(0, 5), (1, 5)]),
        (6, [(0, 6), (1, 6)]),
    ]

    def events(i):
        for when, sends in plan:
            if when == 0:
                continue

            @pl.when(i == when)
            def _(sends=sends):
                send(sends)

    send(plan[0][1])

    def step(i, carry):
        last = i == slots
        inner = lax.rem(i + 1, 2)
        distance = jnp.where(last, 0, half - lax.div(i + 1, 2))
        axes = (jnp.where(last, 0, inner), jnp.where(last, 1, inner))
        places = (distance, jnp.where(last, 0, half + distance))
        compute([start_of(axes[0], distance), start_of(axes[1], -distance)], axes, places, False)
        events(i)
        return carry

    lax.fori_loop(1, side, step, 0)

    share = quarter // side
    order = sorted(range(1, side), key=lambda k: -min(k, side - k))

    def exchange(axis, g, k):
        peer = lax.rem(pos[1 - axis] + k, side)
        rows = pl.ds(pl.multiple_of(quarter * g + peer * share, share), share)
        return pltpu.make_async_remote_copy(
            src_ref=part.at[axis, 0, rows], dst_ref=share_in.at[axis, g, k - 1],
            send_sem=ps_sem.at[axis, g], recv_sem=pr_sem.at[axis, g],
            device_id={"trn": moved(1 - axis, k)},
        )

    def add_mean(axis, k):
        return pltpu.make_async_remote_copy(
            src_ref=mean_own.at[axis], dst_ref=mean_in.at[axis, k - 1],
            send_sem=ms_sem, recv_sem=mr_sem, device_id={"trn": moved(1 - axis, k)},
        )

    def all_of(ref, send_sem, recv_sem):
        return pltpu.make_async_remote_copy(
            src_ref=ref, dst_ref=ref, send_sem=send_sem, recv_sem=recv_sem, device_id={"trn": moved(0, 1)}
        )

    for j in range(2):
        for axis in range(2):
            for way in range(2):
                take(axis, way, slots - 2, 0, j)
    for j in range(2):
        for axis in range(2):
            for way in range(2):
                take(axis, way, slots - 1, 0, j)
                for k in order:
                    exchange(axis, 2 * ((slots - 1 + way) % 2) + j, k).start()
    for axis in range(2):
        mean_own[axis] = part[axis, 0, rank : rank + 1, :]
        for k in order:
            add_mean(axis, k).start()
    for axis in range(2):
        total = jnp.zeros((1, LANES), F32)
        for g in (0, 2, 1, 3):
            all_of(share_in.at[axis, g], ps_sem.at[axis, g], pr_sem.at[axis, g]).wait_recv()
            block = part[axis, 0, pl.ds(pl.multiple_of(quarter * g + pos[1 - axis] * share, share), share), :]
            for k in range(slots):
                block = block + share_in[axis, g, k]
            total = total + jnp.sum(block * block, axis=0, keepdims=True)
        msg[axis : axis + 1, :] = total

    far = lambda k: min(k, side - k)
    others = [(kx, ky) for kx in range(side) for ky in range(side) if (kx, ky) != (0, 0)]

    def spread(kx, ky):
        return pltpu.make_async_remote_copy(
            src_ref=msg, dst_ref=gather.at[me], send_sem=gs_sem, recv_sem=gr_sem,
            device_id={"trn": ring[0][kx] + ring[1][ky]},
        )

    for kx, ky in sorted(others, key=lambda k: -far(k[0]) - far(k[1])):
        spread(kx, ky).start()
    gather[me] = msg[...]

    all_of(mean_in, ms_sem, mr_sem).wait()
    for axis in range(2):
        mean = mean_own[axis]
        for k in range(1, side):
            mean = mean + mean_in[axis, k - 1]
        mean_all[axis, pos[axis]] = mean

    def tell(axis, k):
        return pltpu.make_async_remote_copy(
            src_ref=mean_all.at[axis, pos[axis]], dst_ref=mean_all.at[axis, pos[axis]],
            send_sem=as_sem, recv_sem=ar_sem, device_id={"trn": moved(axis, k)},
        )

    for axis in range(2):
        for k in order:
            tell(axis, k).start()
    for axis in range(2):
        for way in range(2):
            for s in range(slots):
                for j in range(2):
                    hop(axis, way, s, j).wait_send()
        for g in range(4):
            all_of(share_in.at[axis, g], ps_sem.at[axis, g], pr_sem.at[axis, g]).wait_send()
    all_of(mean_all.at[:, pl.ds(0, slots)], as_sem, ar_sem).wait()
    all_of(gather.at[pl.ds(0, side * side - 1)], gs_sem, gr_sem).wait()
    for p in range(side):
        for axis in range(2):
            total = jnp.zeros((2, LANES), F32)
            for q in range(side):
                total = total + gather[q * side + p if axis == 0 else p * side + q]
            row = 2 * p + axis
            out_ref[0, row : row + 1, :] = total[axis : axis + 1]
            out_ref[1, row : row + 1, :] = -mean_all[axis, p]


def on_device(side, test_points, train_points, weights, factor):
    dim, rows = test_points.shape
    local, rank = factor.shape
    slots = side - 1
    share = rank // 4 // side
    chunk = 1024
    dma = pltpu.SemaphoreType.DMA
    out = pl.pallas_call(
        functools.partial(body, side, chunk),
        out_shape=jax.ShapeDtypeStruct((2, rows // LANES, LANES), F32),
        in_specs=[pl.BlockSpec(memory_space=pl.ANY)] * 4,
        out_specs=pl.BlockSpec(memory_space=pltpu.VMEM),
        scratch_shapes=[
            pltpu.VMEM((dim, rows), BF16),
            pltpu.VMEM((dim, local), BF16),
            pltpu.VMEM((local,), BF16),
            pltpu.VMEM((local, rank), BF16),
            pltpu.VMEM((rows, LANES), BF16),
            pltpu.VMEM((LANES, local), BF16),
            pltpu.VMEM((2, side, rank + 8, LANES), F32),
            pltpu.VMEM((2, 2, slots, 2, rank // 4 + 8, LANES), F32),
            pltpu.VMEM((2, 4, slots, share, LANES), F32),
            pltpu.VMEM((2, 1, LANES), F32),
            pltpu.VMEM((2, slots, 1, LANES), F32),
            pltpu.VMEM((2, side, 1, LANES), F32),
            pltpu.VMEM((2, LANES), F32),
            pltpu.VMEM((side * side, 2, LANES), F32),
            dma((3 + local // chunk,)),
            dma((2, 2, slots, 2)), dma((2, 2, slots, 2)),
            dma((2, 4)), dma((2, 4)),
            dma, dma, dma, dma, dma, dma,
        ],
        compiler_params=pltpu.CompilerParams(
            collective_id=0, has_side_effects=True, vmem_limit_bytes=40 * 1024 * 1024
        ),
    )(*(pltpu.with_memory_space_constraint(x, pltpu.HBM) for x in (test_points, train_points, weights, factor)))
    return -out[1].reshape(rows), 1.0 - out[0].reshape(rows)


def solution(mesh):
    side = math.isqrt(mesh.shape["trn"])
    shared = ("grp", "trn")
    return jax.shard_map(
        functools.partial(on_device, side),
        mesh=mesh,
        in_specs=(P(None, ("grp", "tst")), P(None, shared), P(shared), P(shared, None)),
        out_specs=(P(("grp", "tst")), P(("grp", "tst"))),
        check_vma=False,
    )
```

```python
import functools
import math

import jax
import jax.numpy as jnp
from jax import lax
from jax.experimental import pallas as pl
from jax.experimental.pallas import tpu as pltpu
from jax.sharding import PartitionSpec as P

LOG2E = 1.4426950408889634
F32 = jnp.float32
BF16 = jnp.bfloat16
LANES = 128


def pieces_of(value):
    hi = value.astype(BF16).astype(F32)
    rest = value - hi
    mid = rest.astype(BF16).astype(F32)
    low = (rest - mid).astype(BF16).astype(F32)
    return hi, mid, low


def norm_rows(values, ones_first):
    width = values.shape[1]
    row = lax.broadcasted_iota(jnp.int32, (16, width), 0)
    base, ones = (3, 0) if ones_first else (0, 3)
    block = jnp.where((row >= ones) & (row < ones + 3), F32(1), F32(0))
    for k, piece in enumerate(pieces_of(values)):
        block = jnp.where(row == base + k, jnp.broadcast_to(piece, (16, width)), block)
    return block


def half_norms(points):
    points = points.astype(F32)
    return jnp.sum(points * points, axis=0, keepdims=True) * F32(-0.5)


def body(
    side, chunk,
    test_hbm, train_hbm, weight_hbm, factor_hbm, out_ref,
    test, train, weight, factor, lhs, rhs, part, recv, share_in, mean_own, mean_in, mean_all, msg, gather,
    load_sem, s_sem, r_sem, ps_sem, pr_sem, ms_sem, mr_sem, gs_sem, gr_sem, as_sem, ar_sem,
):
    dim, local = train.shape
    rank = factor.shape[1]
    half = side // 2
    slots = side - 1
    wide = 2 * LANES
    turns = local // chunk
    me = lax.axis_index("trn")
    row_pos, col_pos = lax.div(me, side), lax.rem(me, side)
    pos = (col_pos, row_pos)
    ring = [
        [lax.rem(pos[axis] + k, side) * (1, side)[axis] for k in range(side)] for axis in range(2)
    ]

    def moved(axis, k):
        k = k % side
        return ring[0][k] + ring[1][0] if axis == 0 else ring[0][0] + ring[1][k]

    def load(k, src, dst):
        copy = pltpu.make_async_copy(src, dst, load_sem.at[k])
        copy.start()
        return copy

    get_test = load(0, test_hbm, test)
    get_train = load(1, train_hbm, train)
    get_weight = load(2, weight_hbm, weight)

    def load_factor(c):
        rows = pl.ds(c * chunk, chunk)
        return load(3 + c, factor_hbm.at[rows], factor.at[rows])

    get_factor = [load_factor(0)]
    barrier = pltpu.get_barrier_semaphore()
    for axis in range(2):
        for k in (1, -1):
            pl.semaphore_signal(barrier, inc=1, device_id={"trn": moved(axis, k)})

    pad = jnp.zeros((LANES - dim - 16, LANES), F32)
    get_test.wait()
    get_factor += [load_factor(c) for c in range(1, turns)]
    for b in range(test.shape[1] // LANES):
        cols = slice(b * LANES, (b + 1) * LANES)
        points = test[:, cols].astype(F32)
        stack = jnp.concatenate([points, norm_rows(half_norms(points), True), pad], axis=0)
        lhs[cols, :] = stack.T.astype(BF16)
    get_train.wait()
    get_weight.wait()

    quarter = rank // 2
    ends = [quarter * g for g in range(2)] + [rank + 1]
    quarters = [pl.ds(ends[g], ends[g + 1] - ends[g]) for g in range(2)]

    def place(way, distance):
        return distance if way == 0 or distance in (0, half) else half + distance

    def piece(way, s, j):
        return quarters[(s + way) % 2 + j]

    def hop(axis, way, s, j):
        rows = piece(way, s, j)
        return pltpu.make_async_remote_copy(
            src_ref=part.at[axis, place(way, (side - s) // 2), rows],
            dst_ref=recv.at[axis, way, s, j, pl.ds(0, rows.size)],
            send_sem=s_sem.at[axis, way, s, j], recv_sem=r_sem.at[axis, way, s, j],
            device_id={"trn": moved(axis, 1 if way == 0 else -1)},
        )

    def take(axis, way, s, distance, j):
        hop(axis, way, s, j).wait_recv()
        rows = piece(way, s, j)
        at = place(way, distance)
        part[axis, at, rows, :] = part[axis, at, rows, :] + recv[axis, way, s, j, : rows.size, :]

    def send(sends):
        for j in range(1):
            for axis, s in sends:
                for way in range(2):
                    if s >= 2:
                        take(axis, way, s - 2, (side - s) // 2, j)
                    hop(axis, way, s, j).start()

    def compute(starts, axes, places, first):
        points = jnp.concatenate([lhs[pl.ds(s, LANES), :] for s in starts], axis=0)
        total = jnp.zeros((wide, rank), F32)
        weighted = jnp.zeros((wide, LANES), F32)
        kerns = []
        for c in range(turns):
            cols = slice(c * chunk, (c + 1) * chunk)
            if first:
                rhs[:dim, cols] = train[:, cols]
                rhs[dim : dim + 16, cols] = norm_rows(half_norms(train[:, cols]), False).astype(BF16)
                rhs[dim + 16 :, cols] = jnp.zeros((LANES - dim - 16, chunk), BF16)
            power = jnp.dot(points, rhs[:, cols], preferred_element_type=F32)
            kern = jnp.exp2(power * F32(8.0 / dim * LOG2E)).astype(BF16)
            terms = kern.astype(F32) * weight[cols].reshape(1, chunk).astype(F32)
            for g in range(chunk // LANES):
                weighted = weighted + terms[:, g * LANES : (g + 1) * LANES]
            if first:
                kerns.append(kern)
            else:
                total = total + jnp.dot(kern, factor[cols, :], preferred_element_type=F32)
        for c, kern in enumerate(kerns):
            get_factor[c].wait()
            total = total + jnp.dot(kern, factor[c * chunk : (c + 1) * chunk, :], preferred_element_type=F32)
        for k in range(2):
            rows = slice(k * LANES, (k + 1) * LANES)
            part[axes[k], places[k], :rank, :] = total[rows].T
            mean_row = jnp.sum(weighted[rows].T, axis=0, keepdims=True)
            part[axes[k], places[k], rank:, :] = jnp.broadcast_to(mean_row, (8, LANES))

    def start_of(axis, distance):
        at = col_pos if isinstance(axis, int) and axis == 0 else row_pos
        if not isinstance(axis, int):
            at = jnp.where(axis == 0, col_pos, row_pos)
        block = lax.rem(at + distance + side, side)
        return pl.multiple_of((block * 2 + axis) * LANES, LANES)

    compute([start_of(0, half), start_of(1, half)], (0, 1), (half, half), True)
    pl.semaphore_wait(barrier, 4)
    plan = [
        (0, [(0, 0), (1, 0)]),
        (1, [(0, 1)]),
        (2, [(1, 1)]),
        (2, [(0, 2), (1, 2)]),
        (4, [(0, 3), (1, 3)]),
        (5, [(0, 4), (1, 4)]),
        (6, [(0, 5), (1, 5)]),
        (6, [(0, 6), (1, 6)]),
    ]

    def events(i):
        for when, sends in plan:
            if when == 0:
                continue

            @pl.when(i == when)
            def _(sends=sends):
                send(sends)

    send(plan[0][1])

    def step(i, carry):
        last = i == slots
        inner = lax.rem(i + 1, 2)
        distance = jnp.where(last, 0, half - lax.div(i + 1, 2))
        axes = (jnp.where(last, 0, inner), jnp.where(last, 1, inner))
        places = (distance, jnp.where(last, 0, half + distance))
        compute([start_of(axes[0], distance), start_of(axes[1], -distance)], axes, places, False)
        events(i)
        return carry

    lax.fori_loop(1, side, step, 0)

    share = quarter // side
    order = sorted(range(1, side), key=lambda k: -min(k, side - k))

    def exchange(axis, g, k):
        peer = lax.rem(pos[1 - axis] + k, side)
        rows = pl.ds(pl.multiple_of(quarter * g + peer * share, share), share)
        return pltpu.make_async_remote_copy(
            src_ref=part.at[axis, 0, rows], dst_ref=share_in.at[axis, g, k - 1],
            send_sem=ps_sem.at[axis, g], recv_sem=pr_sem.at[axis, g],
            device_id={"trn": moved(1 - axis, k)},
        )

    def add_mean(axis, k):
        return pltpu.make_async_remote_copy(
            src_ref=mean_own.at[axis], dst_ref=mean_in.at[axis, k - 1],
            send_sem=ms_sem, recv_sem=mr_sem, device_id={"trn": moved(1 - axis, k)},
        )

    def all_of(ref, send_sem, recv_sem):
        return pltpu.make_async_remote_copy(
            src_ref=ref, dst_ref=ref, send_sem=send_sem, recv_sem=recv_sem, device_id={"trn": moved(0, 1)}
        )

    for j in range(1):
        for axis in range(2):
            for way in range(2):
                take(axis, way, slots - 2, 0, j)
    for j in range(1):
        for axis in range(2):
            for way in range(2):
                take(axis, way, slots - 1, 0, j)
                for k in order:
                    exchange(axis, (slots - 1 + way) % 2 + j, k).start()
    for axis in range(2):
        mean_own[axis] = part[axis, 0, rank : rank + 1, :]
        for k in order:
            add_mean(axis, k).start()
    for axis in range(2):
        total = jnp.zeros((1, LANES), F32)
        for g in (0, 1):
            all_of(share_in.at[axis, g], ps_sem.at[axis, g], pr_sem.at[axis, g]).wait_recv()
            block = part[axis, 0, pl.ds(pl.multiple_of(quarter * g + pos[1 - axis] * share, share), share), :]
            for k in range(slots):
                block = block + share_in[axis, g, k]
            total = total + jnp.sum(block * block, axis=0, keepdims=True)
        msg[axis : axis + 1, :] = total

    far = lambda k: min(k, side - k)
    others = [(kx, ky) for kx in range(side) for ky in range(side) if (kx, ky) != (0, 0)]

    def spread(kx, ky):
        return pltpu.make_async_remote_copy(
            src_ref=msg, dst_ref=gather.at[me], send_sem=gs_sem, recv_sem=gr_sem,
            device_id={"trn": ring[0][kx] + ring[1][ky]},
        )

    for kx, ky in sorted(others, key=lambda k: -far(k[0]) - far(k[1])):
        spread(kx, ky).start()
    gather[me] = msg[...]

    all_of(mean_in, ms_sem, mr_sem).wait()
    for axis in range(2):
        mean = mean_own[axis]
        for k in range(1, side):
            mean = mean + mean_in[axis, k - 1]
        mean_all[axis, pos[axis]] = mean

    def tell(axis, k):
        return pltpu.make_async_remote_copy(
            src_ref=mean_all.at[axis, pos[axis]], dst_ref=mean_all.at[axis, pos[axis]],
            send_sem=as_sem, recv_sem=ar_sem, device_id={"trn": moved(axis, k)},
        )

    for axis in range(2):
        for k in order:
            tell(axis, k).start()
    for axis in range(2):
        for way in range(2):
            for s in range(slots):
                for j in range(1):
                    hop(axis, way, s, j).wait_send()
        for g in range(2):
            all_of(share_in.at[axis, g], ps_sem.at[axis, g], pr_sem.at[axis, g]).wait_send()
    all_of(mean_all.at[:, pl.ds(0, slots)], as_sem, ar_sem).wait()
    all_of(gather.at[pl.ds(0, side * side - 1)], gs_sem, gr_sem).wait()
    for p in range(side):
        for axis in range(2):
            total = jnp.zeros((2, LANES), F32)
            for q in range(side):
                total = total + gather[q * side + p if axis == 0 else p * side + q]
            row = 2 * p + axis
            out_ref[0, row : row + 1, :] = total[axis : axis + 1]
            out_ref[1, row : row + 1, :] = -mean_all[axis, p]


def on_device(side, test_points, train_points, weights, factor):
    dim, rows = test_points.shape
    local, rank = factor.shape
    slots = side - 1
    share = rank // 2 // side
    chunk = 1024
    dma = pltpu.SemaphoreType.DMA
    out = pl.pallas_call(
        functools.partial(body, side, chunk),
        out_shape=jax.ShapeDtypeStruct((2, rows // LANES, LANES), F32),
        in_specs=[pl.BlockSpec(memory_space=pl.ANY)] * 4,
        out_specs=pl.BlockSpec(memory_space=pltpu.VMEM),
        scratch_shapes=[
            pltpu.VMEM((dim, rows), BF16),
            pltpu.VMEM((dim, local), BF16),
            pltpu.VMEM((local,), BF16),
            pltpu.VMEM((local, rank), BF16),
            pltpu.VMEM((rows, LANES), BF16),
            pltpu.VMEM((LANES, local), BF16),
            pltpu.VMEM((2, side, rank + 8, LANES), F32),
            pltpu.VMEM((2, 2, slots, 1, rank // 2 + 8, LANES), F32),
            pltpu.VMEM((2, 2, slots, share, LANES), F32),
            pltpu.VMEM((2, 1, LANES), F32),
            pltpu.VMEM((2, slots, 1, LANES), F32),
            pltpu.VMEM((2, side, 1, LANES), F32),
            pltpu.VMEM((2, LANES), F32),
            pltpu.VMEM((side * side, 2, LANES), F32),
            dma((3 + local // chunk,)),
            dma((2, 2, slots, 1)), dma((2, 2, slots, 1)),
            dma((2, 2)), dma((2, 2)),
            dma, dma, dma, dma, dma, dma,
        ],
        compiler_params=pltpu.CompilerParams(
            collective_id=0, has_side_effects=True, vmem_limit_bytes=40 * 1024 * 1024
        ),
    )(*(pltpu.with_memory_space_constraint(x, pltpu.HBM) for x in (test_points, train_points, weights, factor)))
    return -out[1].reshape(rows), 1.0 - out[0].reshape(rows)


def solution(mesh):
    side = math.isqrt(mesh.shape["trn"])
    shared = ("grp", "trn")
    return jax.shard_map(
        functools.partial(on_device, side),
        mesh=mesh,
        in_specs=(P(None, ("grp", "tst")), P(None, shared), P(shared), P(shared, None)),
        out_specs=(P(("grp", "tst")), P(("grp", "tst"))),
        check_vma=False,
    )
```
